32 devices in a mesh: part: 2 (over x), data: 4 (over z), model: 4 (over y, core).
Axes of the slice: x: 2, y: 2, z: 4, core: 2. Of those that a mesh axis runs over, the one named last changes fastest.
Arguments:
- x: bfloat16 [2, 8, 2048, 2048], P(None, ('part', 'data'), 'model'), parts along dimension 1
- lengths: int32 [2, 8], P(None, ('part', 'data')), parts along dimension 1
- norm_gain: bfloat16 [2, 2048], P(None, 'data')
- w_in: bfloat16 [2, 2048, 18432], P(None, 'data', 'model')
- w_kv: bfloat16 [2, 2048, 512], P(None, 'data')
- w_out: bfloat16 [2, 10240, 2048], P(None, 'model', 'data')
Outputs:
- output: bfloat16 [2, 8, 2048, 2048], P(None, ('part', 'data'), 'model'), parts along dimension 1
There are 2 independent parts. The reference program is written for one: setup_inputs(seed, part) draws one part's arguments, and reference() takes and returns one part's arrays. A program takes and returns all parts, laid end to end along the dimension named above; an argument that names none is the same for every part.
All inputs are finite; a program needn't handle non-finite values.
Results may differ from the reference program's by a relative error of at most 0.0147284.
Values are sent between devices in bfloat16 or wider.
A program may use at most 1 GiB of HBM per device.

```python
import math
import jax
import jax.numpy as jnp
from jax import lax

N_MICRO = 2
N_LAYERS = 2
N_SEQS = 4
SEQ_LEN = 2048
D_MODEL = 2048
N_HEADS = 8
HEAD_DIM = 256
D_FF = 8192
MODEL_SHARDS = 4
FF_HEAD = D_FF // N_HEADS
UNIT_IN = HEAD_DIM + 2 * FF_HEAD
UNIT_OUT = HEAD_DIM + FF_HEAD
SHARD_ROWS = (N_HEADS // MODEL_SHARDS) * UNIT_OUT
NORM_EPS = 1e-6
NEG_BIG = -1e30
Q_GAIN = math.sqrt(max(math.log(SEQ_LEN / 8.0), 1.0))


def setup_inputs(seed: int = 0, part: int = 0) -> dict:
    part_keys = jax.random.split(jax.random.fold_in(jax.random.key(seed), part), 2)
    shared_keys = jax.random.split(jax.random.key(seed + 1), 4)
    x_act = jax.random.normal(part_keys[0], (N_MICRO, N_SEQS, SEQ_LEN, D_MODEL), jnp.float32)
    seq_lens = jax.random.randint(part_keys[1], (N_MICRO, N_SEQS), SEQ_LEN // 4, SEQ_LEN + 1)
    seq_lens = seq_lens.at[0, 0].set(SEQ_LEN).at[1, 0].set(SEQ_LEN // 4)
    gain_vals = jax.random.uniform(shared_keys[0], (N_LAYERS, D_MODEL), jnp.float32, 0.5, 1.5)
    col_scale = jnp.concatenate([jnp.full((HEAD_DIM,), Q_GAIN, jnp.float32), jnp.ones((2 * FF_HEAD,), jnp.float32)]) * (D_MODEL ** -0.5)
    w_in_vals = jax.random.normal(shared_keys[1], (N_LAYERS, D_MODEL, N_HEADS, UNIT_IN), jnp.float32) * col_scale
    w_kv_vals = jax.random.normal(shared_keys[2], (N_LAYERS, D_MODEL, 2 * HEAD_DIM), jnp.float32) * (D_MODEL ** -0.5)
    row_scale = jnp.concatenate([jnp.full((HEAD_DIM,), (N_HEADS * HEAD_DIM) ** -0.5, jnp.float32), jnp.full((FF_HEAD,), D_FF ** -0.5, jnp.float32)])
    w_out_vals = jax.random.normal(shared_keys[3], (N_LAYERS, N_HEADS, UNIT_OUT, D_MODEL), jnp.float32) * row_scale[:, None]
    return {
        "x": x_act.astype(jnp.bfloat16),
        "lengths": seq_lens.astype(jnp.int32),
        "norm_gain": gain_vals.astype(jnp.bfloat16),
        "w_in": w_in_vals.reshape(N_LAYERS, D_MODEL, N_HEADS * UNIT_IN).astype(jnp.bfloat16),
        "w_kv": w_kv_vals.astype(jnp.bfloat16),
        "w_out": w_out_vals.reshape(N_LAYERS, N_HEADS * UNIT_OUT, D_MODEL).astype(jnp.bfloat16),
    }


def layer_one_seq(x_seq, seq_len, gain_vec, w_in_l, w_kv_l, w_out_l):
    x_f32 = x_seq.astype(jnp.float32)
    centered = x_f32 - jnp.mean(x_f32, axis=-1, keepdims=True)
    variance = jnp.mean(centered * centered, axis=-1, keepdims=True)
    h_act = (centered * lax.rsqrt(variance + NORM_EPS) * gain_vec.astype(jnp.float32)).astype(jnp.bfloat16)
    projected = jnp.dot(h_act, w_in_l, preferred_element_type=jnp.float32).astype(jnp.bfloat16)
    projected = projected.reshape(SEQ_LEN, N_HEADS, UNIT_IN)
    q_heads = projected[:, :, :HEAD_DIM]
    gate_act = projected[:, :, HEAD_DIM:HEAD_DIM + FF_HEAD]
    up_act = projected[:, :, HEAD_DIM + FF_HEAD:]
    kv_act = jnp.dot(h_act, w_kv_l, preferred_element_type=jnp.float32).astype(jnp.bfloat16)
    k_act = kv_act[:, :HEAD_DIM]
    v_act = kv_act[:, HEAD_DIM:]
    scores = jnp.einsum("qhc,kc->hqk", q_heads.astype(jnp.float32), k_act.astype(jnp.float32)) * (1.0 / math.sqrt(HEAD_DIM))
    positions = jnp.arange(SEQ_LEN)
    allowed = (positions[None, :] <= positions[:, None]) & (positions[None, :] < seq_len)
    scores = jnp.where(allowed[None], scores, NEG_BIG)
    attn_probs = jax.nn.softmax(scores, axis=-1).astype(jnp.bfloat16)
    attn_out = jnp.einsum("hqk,kc->qhc", attn_probs.astype(jnp.float32), v_act.astype(jnp.float32)).astype(jnp.bfloat16)
    mlp_out = (jax.nn.silu(gate_act.astype(jnp.float32)) * up_act.astype(jnp.float32)).astype(jnp.bfloat16)
    joined = jnp.concatenate([attn_out, mlp_out], axis=-1).reshape(SEQ_LEN, MODEL_SHARDS, SHARD_ROWS)
    w_groups = w_out_l.reshape(MODEL_SHARDS, SHARD_ROWS, D_MODEL)

    def add_group(running, group_pair):
        rows_in, w_rows = group_pair
        group_sum = jnp.dot(rows_in, w_rows, preferred_element_type=jnp.float32).astype(jnp.bfloat16)
        return running + group_sum.astype(jnp.float32), None

    z_sum, _ = lax.scan(add_group, jnp.zeros((SEQ_LEN, D_MODEL), jnp.float32), (jnp.swapaxes(joined, 0, 1), w_groups))
    return (x_f32 + z_sum).astype(jnp.bfloat16)


def reference(x, lengths, norm_gain, w_in, w_kv, w_out):
    seqs_x = x.reshape(N_MICRO * N_SEQS, SEQ_LEN, D_MODEL)
    seqs_len = lengths.reshape(N_MICRO * N_SEQS)

    def run_seq(seq_item):
        x_seq, seq_len = seq_item

        def one_layer(carry_x, weights):
            gain_l, w_in_l, w_kv_l, w_out_l = weights
            return layer_one_seq(carry_x, seq_len, gain_l, w_in_l, w_kv_l, w_out_l), None

        final_x, _ = lax.scan(one_layer, x_seq, (norm_gain, w_in, w_kv, w_out))
        return final_x

    y_all = lax.map(run_seq, (seqs_x, seqs_len))
    return y_all.reshape(N_MICRO, N_SEQS, SEQ_LEN, D_MODEL)
```

```python
import functools
import math
import jax
import jax.numpy as jnp
from jax import lax
from jax.experimental import pallas as pl
from jax.experimental.pallas import tpu as pltpu
from jax.sharding import PartitionSpec as P

NORM_EPS = 1e-6
NEG_BIG = -1e30
BF16 = jnp.bfloat16
F32 = jnp.float32
VMEM_LIMIT = 67_000_000


def _params(n_axes):
    return pltpu.CompilerParams(dimension_semantics=("arbitrary",) * n_axes, vmem_limit_bytes=VMEM_LIMIT)


def _cost(flops, nbytes, trans=0):
    return pl.CostEstimate(flops=int(flops), bytes_accessed=int(nbytes), transcendentals=int(trans))


def _nbytes(*arrays):
    return sum(math.prod(a.shape) * a.dtype.itemsize for a in arrays)


def _norm_rows(x_f32, gain_row):
    centered = x_f32 - jnp.mean(x_f32, axis=-1, keepdims=True)
    variance = jnp.mean(centered * centered, axis=-1, keepdims=True)
    return (centered * lax.rsqrt(variance + NORM_EPS) * gain_row.astype(F32)).astype(BF16)


def _ln_kernel(x_ref, gain_ref, h_ref):
    h_ref[...] = _norm_rows(x_ref[...].astype(F32), gain_ref[...])


def layer_norm(x_blk, micro, gain):
    _, _, t_loc, d = x_blk.shape
    rows = min(128, t_loc)
    return pl.pallas_call(
        _ln_kernel,
        grid=(t_loc // rows,),
        in_specs=[
            pl.BlockSpec((None, None, rows, d), lambda r: (micro, 0, r, 0)),
            pl.BlockSpec((1, d), lambda r: (0, 0)),
        ],
        out_specs=pl.BlockSpec((rows, d), lambda r: (r, 0)),
        out_shape=jax.ShapeDtypeStruct((t_loc, d), BF16),
        compiler_params=_params(1),
        cost_estimate=_cost(t_loc * d * 8, t_loc * d * 4),
        name="ln",
    )(x_blk, gain)


def _sum_z(x, z_refs, z_dim):
    half = z_refs[0].shape[-1]
    n_half = half // z_dim
    parts = []
    for blk in range(n_half):
        for side in range(2):
            total = None
            for src in range(4):
                term = z_refs[2 * src + side][:, blk * z_dim:(blk + 1) * z_dim].astype(F32)
                total = term if total is None else total + term
            parts.append(total)
    return (x.astype(F32) + jnp.concatenate(parts, axis=-1)).astype(BF16)


def _combine_kernel(z_dim, x_ref, *refs):
    z_refs, gain_ref, y_ref, h_ref = refs[:8], refs[8], refs[9], refs[10]
    y = _sum_z(x_ref[...], z_refs, z_dim)
    y_ref[...] = y
    h_ref[...] = _norm_rows(y.astype(F32), gain_ref[...])


def combine(x_blk, micro, z_list, gain, z_dim):
    _, _, t_loc, d = x_blk.shape
    rows = min(128, t_loc)
    z_spec = pl.BlockSpec((rows, d // 2), lambda r: (r, 0))
    row_spec = pl.BlockSpec((rows, d), lambda r: (r, 0))
    return pl.pallas_call(
        functools.partial(_combine_kernel, z_dim),
        grid=(t_loc // rows,),
        in_specs=[pl.BlockSpec((None, None, rows, d), lambda r: (micro, 0, r, 0))] + [z_spec] * 8
        + [pl.BlockSpec((1, d), lambda r: (0, 0))],
        out_specs=[row_spec, row_spec],
        out_shape=[jax.ShapeDtypeStruct((t_loc, d), BF16)] * 2,
        compiler_params=_params(1),
        cost_estimate=_cost(t_loc * d * 16, t_loc * d * 14),
        name="combine",
    )(x_blk, *z_list, gain)


def _final_kernel(z_dim, x_ref, *refs):
    refs[-1][...] = _sum_z(x_ref[...], refs[:8], z_dim)


def final_combine(x, micro, n_micro, z_list, z_dim, prior):
    t_loc, d = x.shape
    rows = min(128, t_loc)
    z_spec = pl.BlockSpec((rows, d // 2), lambda r: (r, 0))
    extra = [] if prior is None else [prior]
    return pl.pallas_call(
        functools.partial(_final_kernel, z_dim),
        grid=(t_loc // rows,),
        in_specs=[pl.BlockSpec((rows, d), lambda r: (r, 0))] + [z_spec] * 8
        + [pl.BlockSpec(memory_space=pl.ANY)] * len(extra),
        out_specs=pl.BlockSpec((None, None, rows, d), lambda r: (micro, 0, r, 0)),
        out_shape=jax.ShapeDtypeStruct((n_micro, 1, t_loc, d), BF16),
        input_output_aliases={} if prior is None else {9: 0},
        compiler_params=_params(1),
        cost_estimate=_cost(t_loc * d * 8, t_loc * d * 12),
        name="final",
    )(x, *z_list, *extra)


def _pick_kernel(idx_ref, src_ref, dst_ref):
    dst_ref[...] = src_ref[...]


def pick_blocks(idx, gathered):
    n_z, rows, cols = gathered.shape
    return pl.pallas_call(
        _pick_kernel,
        grid_spec=pltpu.PrefetchScalarGridSpec(
            num_scalar_prefetch=1,
            grid=(n_z - 1,),
            in_specs=[pl.BlockSpec((1, rows, cols), lambda j, s: (lax.rem(s[0] + 1 + j, n_z), 0, 0))],
            out_specs=pl.BlockSpec((1, rows, cols), lambda j, s: (j, 0, 0)),
        ),
        out_shape=jax.ShapeDtypeStruct((n_z - 1, rows, cols), BF16),
        compiler_params=_params(1),
        cost_estimate=_cost(rows * cols, 4 * (n_z - 1) * rows * cols),
        name="pick",
    )(idx, gathered)


def _take_kernel(idx_ref, *refs):
    out_ref = refs[-1]
    if len(refs) == 2:
        out_ref[...] = refs[0][0]
    else:
        at = 0
        for src in refs[:-1]:
            out_ref[:, at:at + src.shape[2]] = src[0]
            at += src.shape[2]


def take_blocks(idx, sources, steps):
    rows = sources[0][1][1]
    cols = sum(src[1][2] for src in sources)
    return pl.pallas_call(
        _take_kernel,
        grid_spec=pltpu.PrefetchScalarGridSpec(
            num_scalar_prefetch=1,
            grid=(steps,),
            in_specs=[pl.BlockSpec(shape, index) for _, shape, index in sources],
            out_specs=pl.BlockSpec((rows, cols), lambda t, s: (0, t)),
        ),
        out_shape=jax.ShapeDtypeStruct((rows, cols * steps), BF16),
        compiler_params=_params(1),
        cost_estimate=_cost(rows * cols * steps, 4 * rows * cols * steps),
        name="take",
    )(idx, *[src[0] for src in sources])


def _proj_kernel(gated, tile, kinds, n_h, *refs):
    h_refs = refs[:n_h]
    at = n_h
    w_refs = []
    for kind in kinds:
        width = 3 if kind[1] else 1
        w_refs.append(refs[at:at + width])
        at += width
    n_out = 1 if gated else 2
    outs = refs[at:at + n_out]
    h_scr, w_scr, o_scr, h_sems, w_sems, o_sems = refs[at + n_out:]
    step, last = pl.program_id(0), pl.num_programs(0) - 1
    n_pair, t_loc = n_h // 2, h_scr.shape[1] // 2
    part, z_idx = lax.axis_index("part"), lax.axis_index("data")
    h_copies = [pltpu.make_async_copy(src, h_scr.at[i // 2, pl.ds((i % 2) * t_loc, t_loc)], h_sems.at[i]) for i, src in enumerate(h_refs)]

    def load(at_step):
        slot = lax.rem(at_step, 2)
        start = 0
        for (steps, place), refs_c in zip(kinds, w_refs):
            begin = start

            @pl.when((at_step >= begin) & (at_step < begin + steps))
            def _():
                n = at_step - begin
                cols = pl.ds(pl.multiple_of(n * 2 * tile, 2 * tile), 2 * tile)
                src = refs_c[0]
                n_blk, z_dim, _ = src.shape
                for j in range(n_blk):
                    blk = lax.rem(z_idx + 1 + j, n_blk + 1) if place else j
                    rows = pl.ds(pl.multiple_of(blk * z_dim, z_dim), z_dim)
                    pltpu.make_async_copy(src.at[j, :, cols], w_scr.at[slot, rows], w_sems.at[slot]).start()
                if place:
                    layer, sides = place
                    rows = pl.ds(pl.multiple_of(z_idx * z_dim, z_dim), z_dim)
                    for side in range(2):
                        first = jnp.where(part == 0, sides[side][0], sides[side][1]) + n * tile
                        own = refs_c[1 + side].at[layer, :, pl.ds(pl.multiple_of(first, tile), tile)]
                        pltpu.make_async_copy(own, w_scr.at[slot, rows, pl.ds(side * tile, tile)], w_sems.at[slot]).start()

            start += steps

    def out_copies(at_step, pair):
        slot = lax.rem(at_step, 2)
        cols = pl.ds(pl.multiple_of(at_step * tile, tile), tile)
        return [pltpu.make_async_copy(o_scr.at[slot, k, pl.ds(2 * pair, 2)], out.at[pl.ds(2 * pair, 2), :, cols], o_sems.at[slot, pair]) for k, out in enumerate(outs)]

    @pl.when(step == 0)
    def _():
        load(step)
        for copy in h_copies:
            copy.start()

    @pl.when(step < last)
    def _():
        load(step + 1)

    slot = lax.rem(step, 2)
    pltpu.make_async_copy(w_scr.at[slot], w_scr.at[slot], w_sems.at[slot]).wait()
    for pair in range(n_pair):
        @pl.when(step == 0)
        def _():
            h_copies[2 * pair].wait()
            h_copies[2 * pair + 1].wait()

        @pl.when(step >= 2)
        def _():
            for copy in out_copies(step - 2, pair):
                copy.wait()

        acc = jnp.dot(h_scr[pair], w_scr[slot], preferred_element_type=F32)
        left, right = acc[:, :tile].astype(BF16), acc[:, tile:].astype(BF16)
        shape = (2, t_loc, tile)
        if gated:
            o_scr[slot, 0, pl.ds(2 * pair, 2)] = (jax.nn.silu(left.astype(F32)) * right.astype(F32)).astype(BF16).reshape(shape)
        else:
            o_scr[slot, 0, pl.ds(2 * pair, 2)] = left.reshape(shape)
            o_scr[slot, 1, pl.ds(2 * pair, 2)] = right.reshape(shape)
        for copy in out_copies(step, pair):
            copy.start()

    @pl.when(step == last)
    def _():
        for pair in range(n_pair):
            @pl.when(step >= 1)
            def _():
                for copy in out_copies(step - 1, pair):
                    copy.wait()

            for copy in out_copies(step, pair):
                copy.wait()


def project(pieces, chunks, gated, tile):
    t_loc, d = pieces[0].shape
    n_piece = len(pieces)
    args, kinds, steps = [], [], 0
    for array, *own in chunks:
        n = array.shape[2] // (2 * tile)
        kinds.append((n, own[2] if own else None))
        args += [array] + own[:2]
        steps += n
    n_out = 1 if gated else 2
    out = pl.pallas_call(
        functools.partial(_proj_kernel, gated, tile, tuple(kinds), n_piece),
        grid=(steps,),
        in_specs=[pl.BlockSpec(memory_space=pl.ANY)] * (n_piece + len(args)),
        out_specs=[pl.BlockSpec(memory_space=pl.ANY)] * n_out,
        scratch_shapes=[
            pltpu.VMEM((n_piece // 2, 2 * t_loc, d), BF16),
            pltpu.VMEM((2, d, 2 * tile), BF16),
            pltpu.VMEM((2, n_out, n_piece, t_loc, tile), BF16),
            pltpu.SemaphoreType.DMA((n_piece,)),
            pltpu.SemaphoreType.DMA((2,)),
            pltpu.SemaphoreType.DMA((2, n_piece // 2)),
        ],
        out_shape=[jax.ShapeDtypeStruct((n_piece, t_loc, steps * tile), BF16)] * n_out,
        compiler_params=_params(1),
        cost_estimate=_cost(4 * n_piece * t_loc * d * steps * tile, _nbytes(*pieces) + 4 * d * steps * tile + 2 * n_out * n_piece * t_loc * steps * tile),
        name="proj_gated" if gated else "proj_qkv",
    )(*pieces, *args)
    return out[0] if gated else out


def _attn_kernel(idx_ref, len_ref, *refs):
    q_a, q_b, kv_a, kv_b, o_ref, k_scr, v_scr, s_scr, p_scr = refs
    head, slot, row = pl.program_id(0), pl.program_id(1), pl.program_id(2)
    part, me = idx_ref[1], idx_ref[2]
    n_blk, blk, head_dim = kv_a.shape
    bq = q_a.shape[1]

    @pl.when((head == 0) & (slot == 0) & (row == 0))
    def _():
        for k in range(n_blk):
            rows = pl.ds(pl.multiple_of((me ^ k) * blk, blk), blk)
            first, second = kv_a[k], kv_b[k]
            k_scr[rows, :] = jnp.where(part == 0, first, second)
            v_scr[rows, :] = jnp.where(part == 0, second, first)

    q = jnp.where(head == 0, q_a[0], q_b[0])
    q_blk = me ^ slot
    seq_len = len_ref[0]
    n_keys = jnp.minimum(q_blk + 1, (seq_len + blk - 1) // blk)
    rate = math.log2(math.e) / math.sqrt(head_dim)
    lane = min(128, blk)

    def fold(x, op):
        total = x[:, :lane]
        for i in range(1, x.shape[1] // lane):
            total = op(total, x[:, i * lane:(i + 1) * lane])
        return total

    for n in range(1, n_blk + 1):
        @pl.when(n_keys == n)
        def _():
            top = None
            for j in range(n):
                s = lax.dot_general(q, k_scr[j * blk:(j + 1) * blk, :], (((1,), (1,)), ((), ())), preferred_element_type=F32)
                if j == n - 1:
                    q_pos = q_blk * blk + row * bq + lax.broadcasted_iota(jnp.int32, (bq, blk), 0)
                    k_pos = j * blk + lax.broadcasted_iota(jnp.int32, (bq, blk), 1)
                    s = jnp.where(k_pos <= jnp.minimum(q_pos, seq_len - 1), s, NEG_BIG)
                s_scr[:, j * blk:(j + 1) * blk] = s
                part_top = fold(s, jnp.maximum)
                top = part_top if top is None else jnp.maximum(top, part_top)
            top = jnp.max(top, axis=-1, keepdims=True)
            total = None
            for j in range(n):
                e = jnp.exp2((s_scr[:, j * blk:(j + 1) * blk] - top) * rate)
                s_scr[:, j * blk:(j + 1) * blk] = e
                part_sum = fold(e, jnp.add)
                total = part_sum if total is None else total + part_sum
            inv = 1.0 / jnp.sum(total, axis=-1, keepdims=True)
            for j in range(n):
                p_scr[:, j * blk:(j + 1) * blk] = (s_scr[:, j * blk:(j + 1) * blk] * inv).astype(BF16)
            o_ref[0] = jnp.dot(p_scr[:, :n * blk], v_scr[:n * blk, :], preferred_element_type=F32).astype(BF16)


def attention(idx, seq_len, q_a, q_b, kv_a, kv_b):
    head_dim = q_a[3]
    _, blk, _ = q_a[0].shape
    n_blk = 4
    bq = min(256, blk)
    n_row = blk // bq

    def q_spec(item, which):
        _, col, first, _ = item
        hold = 0 if which else n_blk - 1, 0 if which else n_row - 1
        return pl.BlockSpec((1, bq, head_dim), lambda a, k, r, s, t: (first + jnp.where(a == which, k, hold[0]), jnp.where(a == which, r, hold[1]), col))

    def kv_spec(item):
        _, col, first, _ = item
        return pl.BlockSpec((n_blk, blk, head_dim), lambda a, k, r, s, t: (first // n_blk, 0, col))

    return pl.pallas_call(
        _attn_kernel,
        grid_spec=pltpu.PrefetchScalarGridSpec(
            num_scalar_prefetch=2,
            grid=(2, n_blk, n_row),
            in_specs=[q_spec(q_a, 0), q_spec(q_b, 1), kv_spec(kv_a), kv_spec(kv_b)],
            out_specs=pl.BlockSpec((1, bq, head_dim), lambda a, k, r, s, t: (n_blk * a + k, r, 0)),
            scratch_shapes=[
                pltpu.VMEM((n_blk * blk, head_dim), BF16),
                pltpu.VMEM((n_blk * blk, head_dim), BF16),
                pltpu.VMEM((bq, n_blk * blk), F32),
                pltpu.VMEM((bq, n_blk * blk), BF16),
            ],
        ),
        out_shape=jax.ShapeDtypeStruct((2 * n_blk, blk, head_dim), BF16),
        compiler_params=_params(3),
        cost_estimate=_cost(8 * (n_blk * blk) ** 2 * head_dim * 0.8, 12 * n_blk * blk * head_dim, (n_blk * blk) ** 2),
        name="attn",
    )(idx, seq_len, q_a[0], q_b[0], kv_a[0], kv_b[0])


def _out_kernel(layer, side, items, n_in, *refs):
    srcs = refs[:n_in]
    wa_ref, own_ref, rel_ref = refs[n_in:n_in + 3]
    z_refs = refs[n_in + 3:n_in + 7]
    j_scr, w_scr, z_scr, j_sems, w_sems, z_sems = refs[n_in + 7:]
    step, last = pl.program_id(0), pl.num_programs(0) - 1
    t_loc = j_scr.shape[1] // 2
    n_z, rows, width = wa_ref.shape
    part, z_idx = lax.axis_index("part"), lax.axis_index("data")
    order = (2, 3, 0, 1)
    copies = []
    for i, slot in enumerate(order):
        at, mine = 0, []
        for head in range(2):
            for low, high, first_low, first_high, col, size in items[head]:
                ref, first = (srcs[low], first_low) if slot < 2 else (srcs[high], first_high)
                src = ref.at[first + slot, :, pl.ds(col, size)]
                mine.append(pltpu.make_async_copy(src, j_scr.at[i // 2, pl.ds((i % 2) * t_loc, t_loc), pl.ds(at, size)], j_sems.at[i // 2]))
                at += size
        copies.append(mine)

    def load(at_step):
        for i in range(2):
            blk = 2 * at_step + i
            cols = pl.ds(i * width, width)
            pltpu.make_async_copy(wa_ref.at[blk], w_scr.at[at_step, pl.ds(0, rows), cols], w_sems.at[at_step]).start()
            below = w_scr.at[at_step, pl.ds(rows, rows), cols]

            @pl.when(blk == z_idx)
            def _():
                first = pl.multiple_of((1 - part) * rows, rows)
                pltpu.make_async_copy(own_ref.at[layer, pl.ds(first, rows), pl.ds(side * width, width)], below, w_sems.at[at_step]).start()

            @pl.when(blk != z_idx)
            def _():
                pltpu.make_async_copy(rel_ref.at[lax.rem(blk - z_idx - 1 + n_z, n_z)], below, w_sems.at[at_step]).start()

    def z_copies(at_step, pair):
        cols = pl.ds(pl.multiple_of(at_step * 2 * width, 2 * width), 2 * width)
        return [pltpu.make_async_copy(z_scr.at[at_step, pair, pl.ds(k * t_loc, t_loc)], z_refs[order[2 * pair + k]].at[:, cols], z_sems.at[at_step, pair]) for k in range(2)]

    @pl.when(step == 0)
    def _():
        load(0)
        for mine in copies[:2]:
            for copy in mine:
                copy.start()
        load(1)
        for mine in copies[2:]:
            for copy in mine:
                copy.start()

    pltpu.make_async_copy(w_scr.at[step], w_scr.at[step], w_sems.at[step]).wait()
    for pair in range(2):
        @pl.when(step == 0)
        def _():
            for mine in copies[2 * pair:2 * pair + 2]:
                for copy in mine:
                    copy.wait()

        z_scr[step, pair] = jnp.dot(j_scr[pair], w_scr[step], preferred_element_type=F32).astype(BF16)
        for copy in z_copies(step, pair):
            copy.start()

    @pl.when(step == last)
    def _():
        for at_step in range(2):
            for pair in range(2):
                for copy in z_copies(at_step, pair):
                    copy.wait()


def out_project(layer, side, items, srcs, w_a, w_own, w_rel):
    n_z, rows, z_dim = w_a.shape
    n_slot, t_loc = 4, srcs[0].shape[1]
    steps = n_z // 2
    return pl.pallas_call(
        functools.partial(_out_kernel, layer, side, items, len(srcs)),
        grid=(steps,),
        in_specs=[pl.BlockSpec(memory_space=pl.ANY)] * (len(srcs) + 3),
        out_specs=[pl.BlockSpec(memory_space=pl.ANY)] * n_slot,
        scratch_shapes=[
            pltpu.VMEM((n_slot // 2, 2 * t_loc, 2 * rows), BF16),
            pltpu.VMEM((steps, 2 * rows, 2 * z_dim), BF16),
            pltpu.VMEM((steps, n_slot // 2, 2 * t_loc, 2 * z_dim), BF16),
            pltpu.SemaphoreType.DMA((2,)),
            pltpu.SemaphoreType.DMA((steps,)),
            pltpu.SemaphoreType.DMA((steps, 2)),
        ],
        out_shape=[jax.ShapeDtypeStruct((t_loc, n_z * z_dim), BF16)] * n_slot,
        compiler_params=_params(1),
        cost_estimate=_cost(4 * n_slot * t_loc * rows * n_z * z_dim, 4 * n_slot * t_loc * rows + 4 * rows * n_z * z_dim + 2 * n_slot * t_loc * n_z * z_dim),
        name="out_proj",
    )(*srcs, w_a, w_own, w_rel)


def _swap(value, axis, size, k):
    return lax.ppermute(value, axis, [(i, i ^ k) for i in range(size)])


TAKE, PICK, GAIN, NORM, FORWARD, QKV, ATTEND, GATE, OUT, JOIN, FINAL = (
    "take", "pick", "gain", "norm", "forward", "qkv", "attend", "gate", "out", "join", "final")

ORDER = [
    (TAKE, "00"), (GAIN, ""), (NORM, "0"), (NORM, "1"), *[(TAKE, f"0{c}") for c in "1234"], *[(TAKE, f"1{c}") for c in "01234"],
    (FORWARD, "00"), (PICK, "00"), (QKV, "0", "0", "a"), (FORWARD, "01"), (QKV, "0", "0", "b"), (QKV, "0", "1", "a"), (PICK, "01"),
    (QKV, "0", "1", "b"), (ATTEND, "00"), (ATTEND, "01"), (GATE, "0", "01", "a0"), (PICK, "02"), (GATE, "0", "01", "b0"),
    (GATE, "0", "01", "a1"), (PICK, "03"), (GATE, "0", "01", "b1"), (PICK, "04"),
    (OUT, "000"), (PICK, "10"), (OUT, "001"), (OUT, "010"), (JOIN, "00"), (PICK, "11"), (OUT, "011"), (FORWARD, "10"),
    (QKV, "1", "0", "ab"), (ATTEND, "10"), (PICK, "12"), (GATE, "1", "0", "a0b0a1"), (JOIN, "01"), (PICK, "13"), (GATE, "1", "0", "b1"),
    (GATE, "1", "1", "a0b0a1b1", "lo"), (PICK, "14"), (OUT, "100"), (FORWARD, "11"), (QKV, "1", "1", "ab"), (ATTEND, "11"), (OUT, "101"),
    (GATE, "1", "1", "a0b0a1b1", "hi"), (OUT, "110"), (OUT, "111"), (FINAL, "0"), (FINAL, "1"),
]


def build(mesh):
    n_part, n_data, n_model = mesh.shape["part"], mesh.shape["data"], mesh.shape["model"]
    act_spec = P(None, ("part", "data"), "model", None)

    def local_fn(x_blk, len_blk, gain_blk, w_in_blk, w_kv_blk, w_out_blk):
        n_micro, _, t_loc, d = x_blk.shape
        n_layers, z_dim, in_loc = w_in_blk.shape
        head_dim = w_kv_blk.shape[2] // 2
        unit_out = w_out_blk.shape[1] // 2
        ff = unit_out - head_dim
        unit_in = in_loc // 2
        n_chunk = 2
        ff_c = ff // n_chunk
        tile = min(256, ff_c)
        per_chunk = ff_c // tile
        z_half = z_dim // 2
        z_idx = lax.axis_index("data")
        idx = jnp.stack([z_idx, lax.axis_index("part"), lax.axis_index("model")]).astype(jnp.int32)

        now = [idx]

        def seq(value):
            now[0], value = lax.optimization_barrier((now[0], value))
            return value

        def tied(value):
            return lax.optimization_barrier((value, now[0]))[0]

        def q_map(layer):
            return lambda n, s: (layer, 0, s[1] * (unit_in // head_dim))

        def kv_map(layer):
            return lambda n, s: (layer, 0, s[1])

        def gate_map(layer, c, up):
            return lambda n, s: (layer, 0, (s[1] * unit_in + head_dim + (ff if up else 0) + c * ff_c) // tile + n)

        def out_map(layer, side):
            return lambda n, s: (layer, s[1], side)

        gathered, rel = {}, {}

        def take(at):
            layer, c = map(int, at)
            if c == 0:
                sources = [(w_in_blk, (1, z_dim, head_dim), q_map(layer)), (w_kv_blk, (1, z_dim, head_dim), kv_map(layer))]
                steps = 1
            elif c <= n_chunk:
                sources = [(w_in_blk, (1, z_dim, tile), gate_map(layer, c - 1, up)) for up in (False, True)]
                steps = per_chunk
            else:
                sources = [(w_out_blk, (1, unit_out, z_half), out_map(layer, c - 1 - n_chunk))]
                steps = 1
            mine = seq(take_blocks(now[0], sources, steps))
            gathered[layer, c] = lax.all_gather(mine, "data", axis=0)

        def pick(at):
            layer, c = map(int, at)
            send = seq(pick_blocks(now[0], gathered[layer, c]))
            rel[layer, c] = _swap(send, "part", n_part, 1)

        hs, near, far, both = {}, {}, {}, {}

        def spread(layer, m, h):
            hs[layer, m] = h
            far[layer, m] = _swap(h, "model", n_model, 2)
            near[layer, m] = _swap(h, "model", n_model, 1)

        def forward(at):
            layer, m = map(int, at)
            far[layer, m] = seq(far[layer, m])
            both[layer, m] = _swap(far[layer, m], "model", n_model, 1)

        q, kv, attn, mid, zs = {}, {}, {}, {}, {}

        def pieces(layer, micros, slots="lohi"):
            found = []
            for m in map(int, micros):
                found += [hs[layer, m], near[layer, m]] if "lo" in slots else []
                found += [far[layer, m], both[layer, m]] if "hi" in slots else []
            return [tied(found[0])] + found[1:]

        def qkv(layer, micros, names):
            layer = int(layer)
            chunks = []
            for name in names:
                if name == "a":
                    chunks.append((gathered[layer, 0],))
                else:
                    chunks.append((rel[layer, 0], w_in_blk, w_kv_blk, (layer, ((unit_in, 0), (head_dim, 0)))))
            q_out, kv_out = seq(project(pieces(layer, micros), chunks, False, head_dim))
            for i, m in enumerate(map(int, micros)):
                for col, name in enumerate(names):
                    q[layer, m, name] = (q_out, col, n_model * i, head_dim)
                    kv[layer, m, name] = (kv_out, col, n_model * i, head_dim)

        def attend(at):
            layer, m = map(int, at)
            attn[layer, m] = seq(attention(now[0], len_blk[m], q[layer, m, "a"], q[layer, m, "b"], kv[layer, m, "a"], kv[layer, m, "b"]))

        def gate(layer, micros, names, slots="lohi"):
            layer = int(layer)
            chunks = []
            names = [names[i:i + 2] for i in range(0, len(names), 2)]
            for head, c in names:
                c = int(c)
                if head == "a":
                    chunks.append((gathered[layer, 1 + c],))
                else:
                    gate_at = head_dim + c * ff_c
                    up_at = gate_at + ff
                    chunks.append((rel[layer, 1 + c], w_in_blk, w_in_blk, (layer, ((unit_in + gate_at, gate_at), (unit_in + up_at, up_at)))))
            got = seq(project(pieces(layer, micros, slots), chunks, True, tile))
            for i, m in enumerate(map(int, micros)):
                for col, name in enumerate(names):
                    for part_of in ("lo", "hi"):
                        if part_of in slots:
                            first = n_model * i if slots == "lohi" else (0 if slots == "lo" else -2)
                            mid[layer, m, name, part_of] = (got, first, col * ff_c)

        def out(at):
            layer, m, side = map(int, at)
            c = 1 + n_chunk + side
            srcs = [tied(attn[layer, m])]

            def operand(array):
                for i, known in enumerate(srcs):
                    if known is array:
                        return i
                srcs.append(array)
                return len(srcs) - 1

            items = []
            for number, head in enumerate("ab"):
                row = [(0, 0, n_model * number, n_model * number, 0, head_dim)]
                for i in range(n_chunk):
                    low, high = mid[layer, m, f"{head}{i}", "lo"], mid[layer, m, f"{head}{i}", "hi"]
                    row.append((operand(low[0]), operand(high[0]), low[1], high[1], low[2], ff_c))
                items.append(tuple(row))
            values = seq(out_project(layer, side, tuple(items), srcs, gathered[layer, c], w_out_blk, rel[layer, c]))
            for k in (0, 2, 3, 1):
                zs[layer, m, k, side] = values[k] if k == 0 else _swap(values[k], "model", n_model, k)

        ys = {}

        def z_list(layer, m):
            return [zs[layer, m, k, side] for k in range(n_model) for side in range(2)]

        gain_full = [None]

        def gain(_):
            blk = tied(gain_blk)
            got = [blk] + [_swap(blk, "data", n_data, k) for k in range(1, n_data)]
            blocks = []
            for b in range(n_data):
                choice = got[n_data - 1]
                for k in range(n_data - 1):
                    choice = jnp.where((z_idx ^ k) == b, got[k], choice)
                blocks.append(choice)
            gain_full[0] = jnp.concatenate(blocks, axis=1)

        def join(at):
            layer, m = map(int, at)
            src, place = (x_blk, m) if layer == 0 else (ys[layer - 1, m].reshape(1, 1, t_loc, d), 0)
            row = tied(gain_full[0][layer + 1:layer + 2])
            ys[layer, m], h = seq(combine(src, place, z_list(layer, m), row, z_half))
            spread(layer + 1, m, h)

        def norm(at):
            m = int(at)
            spread(0, m, seq(layer_norm(x_blk, m, tied(gain_full[0][0:1]))))

        result = [None]

        def final(at):
            m = int(at)
            result[0] = seq(final_combine(ys[n_layers - 2, m], m, n_micro, z_list(n_layers - 1, m), z_half, result[0]))

        steps = {TAKE: take, PICK: pick, GAIN: gain, NORM: norm, FORWARD: forward, QKV: qkv, ATTEND: attend, GATE: gate, OUT: out, JOIN: join, FINAL: final}
        for step in ORDER:
            steps[step[0]](*step[1:])
        return result[0]

    return jax.shard_map(
        local_fn,
        mesh=mesh,
        in_specs=(act_spec, P(None, ("part", "data")), P(None, "data"), P(None, "data", "model"), P(None, "data", None), P(None, "model", "data")),
        out_specs=act_spec,
        check_vma=False,
    )


def solution(mesh):
    return build(mesh)
```
